128 devices in a mesh: expert: 16 (over z, x), tensor: 4 (over y), dp: 2 (over core).
Axes of the slice: x: 4, y: 4, z: 4, core: 2. Of those that a mesh axis runs over, the one named last changes fastest.
Arguments:
- tokens: bfloat16 [16384, 2048], P(('dp', 'expert', 'tensor')), parts along dimension 0, may hold values from -6 to 6
- expert_ids: int32 [16384, 4], P(('dp', 'expert', 'tensor')), parts along dimension 0, may hold values from 0 to 63, all different within a row; in each aligned block of 128 rows (0 to 127, 128 to 255, ...) at most 16 rows name the same one
- gate_probs: float32 [16384, 4], P(('dp', 'expert', 'tensor')), parts along dimension 0, may hold values from 0.05 to 0.6
- w_gate: bfloat16 [64, 2048, 1408], P(('expert', 'tensor')), may hold values from -0.125 to 0.125
- w_up: bfloat16 [64, 2048, 1408], P(('expert', 'tensor')), may hold values from -0.125 to 0.125
- w_down: bfloat16 [64, 1408, 2048], P(('expert', 'tensor')), may hold values from -0.15625 to 0.15625
- s_gate: bfloat16 [2048, 2816], P(None, 'tensor'), may hold values from -0.125 to 0.125
- s_up: bfloat16 [2048, 2816], P(None, 'tensor'), may hold values from -0.125 to 0.125
- s_down: bfloat16 [2816, 2048], P('tensor'), may hold values from -0.109375 to 0.109375
- shared_gate: bfloat16 [2048], replicated, may hold values from -0.125 to 0.125
Outputs:
- mixed: bfloat16 [16384, 2048], P(('dp', 'expert', 'tensor')), parts along dimension 0
The draws below stay inside these ranges and needn't reach their ends.
There are 2 independent parts, one for each index of `dp`. The reference program is written for one: setup_inputs(seed, part) draws one part's arguments, and reference() takes and returns one part's arrays. A program takes and returns all parts, laid end to end along the dimension named above; an argument that names none is the same for every part. Nothing has to cross between parts.
Inputs may be any that keep to these rules, and one draw needn't show every extreme that they name: `expert_ids`: among the rows of one device, no expert is named by more than 16 of them.
All inputs are finite; a program needn't handle non-finite values.
Results may differ from the reference program's by a relative error of at most 0.0095.
Values may be sent and summed in bfloat16 or wider, within the bound.
No kernel may reach another device: no remote copies, remote signals or barrier semaphores. Data moves between devices by JAX's collectives and lax.ppermute only.
A program may use at most 128 MiB of HBM per device.

```python
import math
import jax
import jax.numpy as jnp
import numpy as np
from jax import lax

D = 2048
F = 1408
FS = 2816
TOP = 4
TOK_DEV = 128
EXPERTS = 64
CAP = 16
TOKENS = 8192
N_EXPERT = 16
N_TENSOR = 4


def level_of(rng, extent, shards, least, largest):
    factor_of = 1.0
    for position, blocks in shards:
        draws = jax.random.uniform(jax.random.fold_in(jax.random.fold_in(rng, 6), position), (blocks,), jnp.float32, least / len(shards), largest / len(shards))
        factor_of = factor_of * jnp.repeat(jnp.exp(draws), extent[position] // blocks).reshape((-1,) + (1,) * (len(extent) - 1 - position))
    return factor_of


def assign_block(own_key, own, number, rows, amount, top, bound, slope):
    sequence = jax.random.permutation(own_key, amount)
    crowded, common = load_shares(amount, rows * top, bound, slope, True), load_shares(amount, rows * top, bound, slope, False)
    places = jnp.arange(amount)

    def named(lengths, rotation):
        used = int((lengths > 0).sum())
        fixed = max(1, used // 4)
        shifted = fixed + (places - fixed + rotation * (used - fixed)) % max(1, amount - fixed)
        return jnp.zeros((amount,), jnp.int32).at[sequence[jnp.where(places < fixed, places, shifted)]].set(jnp.asarray(lengths, jnp.int32))

    lengths = jnp.where(number % 4 == 0, named(crowded, number // 4), named(common, number - number // 4 - 1))
    mixed = jax.random.permutation(jax.random.fold_in(own, 3), amount)
    donor, taker = mixed[0:amount // 2 * 2:2], mixed[1:amount // 2 * 2:2]
    room = jnp.minimum(lengths[donor] - 1, bound - lengths[taker]) // 2
    room = jnp.where((donor == sequence[0]) | (taker == sequence[0]) | (lengths[taker] == 0), 0, jnp.maximum(room, 0))
    shifted = jax.random.randint(jax.random.fold_in(own, 4), (amount // 2,), 0, 1 << 20) % (room + 1)
    lengths = lengths.at[donor].add(-shifted).at[taker].add(shifted)
    items = jnp.searchsorted(jnp.cumsum(lengths), jnp.arange(rows * top), side="right").astype(jnp.int32)
    grid = items.reshape(top, rows).T
    grid = grid[jax.random.permutation(jax.random.fold_in(own, 1), rows)]
    rotation = jax.random.randint(jax.random.fold_in(own, 2), (rows, 1), 0, top)
    return jnp.take_along_axis(grid, (jnp.arange(top)[None, :] + rotation) % top, axis=1)


def load_shares(number_of, total, most, skew, full):
    weights = [(1 << 20) // math.isqrt(grade ** skew) + 1 for grade in range(1, number_of + 1)]
    largest = most if full else min(most, max(-(-total // number_of), total * weights[0] // sum(weights)))
    least = 1 if total - largest >= number_of - 1 else 0
    holding, spare = [largest] + [least] * (number_of - 1), total - largest - least * (number_of - 1)
    while spare > 0:
        candidates = [i for i in range(1, number_of) if holding[i] < largest] or [i for i in range(1, number_of) if holding[i] < most]
        mass, remaining = sum([weights[i] for i in candidates]), spare
        for i in candidates:
            addition = min(most - holding[i], max(1, remaining * weights[i] // mass), spare)
            holding[i] = holding[i] + addition
            spare = spare - addition
    return np.array(holding)


def normal_values(rng, dims, spread, most, pieces=(), kind=jnp.bfloat16):
    drawn = spread * jax.random.normal(rng, dims, jnp.float32)
    if pieces:
        drawn = drawn * level_of(rng, dims, pieces, -0.22, 0.18)
    return jnp.clip(drawn, -most, most).astype(kind)


def setup_inputs(seed: int = 0, part: int = 0) -> dict:
    arg_keys = jax.random.split(jax.random.key(seed), 11)
    part_splits = jax.random.split(jax.random.fold_in(arg_keys[10], part), 11)
    tokens = normal_values(part_splits[0], (TOKENS, D), 1.0, 6.0, ((0, 64),))
    expert_ids_keys = jax.random.split(jax.random.fold_in(part_splits[1], 1), TOKENS // TOK_DEV)
    expert_ids_turns = jax.random.permutation(jax.random.fold_in(part_splits[1], 3), TOKENS // TOK_DEV)
    expert_ids = jax.vmap(lambda own, number: assign_block(jax.random.fold_in(part_splits[1], 2), own, number, TOK_DEV, EXPERTS, TOP, CAP, 2))(expert_ids_keys, expert_ids_turns).reshape((TOKENS, TOP))
    gate_probs = jnp.clip(jnp.exp(math.log(0.6) - 2.4849067 * jax.random.uniform(part_splits[2], (TOKENS, TOP), jnp.float32) ** level_of(part_splits[2], (TOKENS, TOP), ((0, 64),), -0.2, 0.2)), 0.05, 0.6)
    w_gate = normal_values(arg_keys[3], (EXPERTS, D, F), D ** -0.5, 0.125, ((0, 64),))
    w_up = normal_values(arg_keys[4], (EXPERTS, D, F), D ** -0.5, 0.125, ((0, 64),))
    w_down = normal_values(arg_keys[5], (EXPERTS, F, D), F ** -0.5, 0.15625, ((0, 64),))
    s_gate = normal_values(arg_keys[6], (D, FS), D ** -0.5, 0.125, ((1, 4),))
    s_up = normal_values(arg_keys[7], (D, FS), D ** -0.5, 0.125, ((1, 4),))
    s_down = normal_values(arg_keys[8], (FS, D), FS ** -0.5, 0.109375, ((0, 4),))
    shared_gate = normal_values(arg_keys[9], (D,), D ** -0.5, 0.125)
    return dict(tokens=tokens, expert_ids=expert_ids, gate_probs=gate_probs, w_gate=w_gate, w_up=w_up, w_down=w_down, s_gate=s_gate, s_up=s_up, s_down=s_down, shared_gate=shared_gate)


def silu_product(rows, w_first, w_second):
    gate = jnp.dot(rows, w_first, preferred_element_type=jnp.float32)
    up = jnp.dot(rows, w_second, preferred_element_type=jnp.float32)
    return (jax.nn.silu(gate) * up).astype(jnp.bfloat16)


def slot_index(ids, experts, capacity):
    flat = ids.reshape(-1).astype(jnp.int32)
    onehot = (flat[:, None] == jnp.arange(experts, dtype=jnp.int32)[None, :]).astype(jnp.int32)
    before = jnp.cumsum(onehot, axis=0) - onehot
    return (flat * capacity + jnp.sum(before * onehot, axis=1)).astype(jnp.int32)


def reference(tokens, expert_ids, gate_probs, w_gate, w_up, w_down, s_gate, s_up, s_down, shared_gate):
    sources = N_EXPERT * N_TENSOR
    blocks = tokens.reshape(sources, TOK_DEV, D)
    slots = jax.vmap(lambda ids: slot_index(ids, EXPERTS, CAP))(expert_ids.reshape(sources, TOK_DEV, TOP))
    repeated = jnp.repeat(blocks, TOP, axis=1)

    def fill(rows, slot):
        return jnp.zeros((EXPERTS * CAP, D), jnp.bfloat16).at[slot].set(rows)

    sent = jax.vmap(fill)(repeated, slots)
    grouped = sent.reshape(sources, EXPERTS, CAP, D).transpose(1, 0, 2, 3).reshape(EXPERTS, sources * CAP, D)

    def run_expert(packed_args):
        rows, first, second, third = packed_args
        hidden = silu_product(rows, first, second)
        return jnp.dot(hidden, third, preferred_element_type=jnp.float32).astype(jnp.bfloat16)

    finished = lax.map(run_expert, (grouped, w_gate, w_up, w_down))
    returned = finished.reshape(EXPERTS, sources, CAP, D).transpose(1, 0, 2, 3).reshape(sources, EXPERTS * CAP, D)
    picked = jax.vmap(lambda outs, slot: outs[slot])(returned, slots).reshape(TOKENS, TOP, D)
    routed = jnp.einsum("tk,tkd->td", gate_probs.astype(jnp.float32), picked.astype(jnp.float32))
    hidden = silu_product(tokens, s_gate, s_up)
    group = FS // N_TENSOR
    shared = jnp.zeros((TOKENS, D), jnp.float32)
    for member in range(N_TENSOR):
        part = jnp.dot(hidden[:, member * group:(member + 1) * group], s_down[member * group:(member + 1) * group], preferred_element_type=jnp.float32)
        shared = shared + part.astype(jnp.bfloat16).astype(jnp.float32)
    scale = jax.nn.sigmoid(jnp.dot(tokens, shared_gate, preferred_element_type=jnp.float32))
    return (scale[:, None] * shared + routed).astype(jnp.bfloat16)
```

```python
import functools

import jax
import jax.numpy as jnp
from jax import lax
from jax.experimental import pallas as pl
from jax.experimental.pallas import tpu as pltpu
from jax.sharding import PartitionSpec as P


BF16 = jnp.bfloat16
F32 = jnp.float32
VMEM = pl.BlockSpec(memory_space=pltpu.VMEM)
HBM = pl.BlockSpec(memory_space=pltpu.HBM)
LARGE = 60 * 1024 * 1024


def dot(a, b):
    return jnp.dot(a, b, preferred_element_type=F32)


def tdot(a, b):
    return lax.dot_general(a, b, (((0,), (0,)), ((), ())), preferred_element_type=F32)


def ndot(a, b):
    return lax.dot_general(a, b, (((1,), (1,)), ((), ())), preferred_element_type=F32)


def fetch(pairs, sems):
    copies = [pltpu.make_async_copy(a, b, sems.at[i]) for i, (a, b) in enumerate(pairs)]
    for c in copies:
        c.start()
    return copies


def finish(copies):
    for c in copies:
        c.wait()


def weigh(meta, shape, mine, members):
    groups, capacity, rows = shape
    top = meta.shape[0] // 2
    earlier = lax.broadcasted_iota(jnp.int32, (rows, rows), 0)
    later = lax.broadcasted_iota(jnp.int32, (rows, rows), 1)
    before = (earlier < later).astype(BF16)
    expert = lax.broadcasted_iota(jnp.int32, (groups, rows), 0).astype(F32) * members + mine
    place = lax.broadcasted_iota(jnp.int32, shape, 1).astype(F32)
    named = jnp.zeros((groups, rows), F32)
    prob = jnp.zeros((groups, rows), F32)
    for k in range(top):
        hit = meta[k : k + 1] == expert
        named = jnp.where(hit, 1.0, named)
        prob = jnp.where(hit, meta[top + k : top + k + 1], prob)
    rank = dot(named.astype(BF16), before)
    slot = jnp.where(named > 0.0, rank, -1.0)
    pick = slot[:, None, :] == place
    high = prob.astype(BF16).astype(F32)
    low = prob - high

    def spread(value):
        wide = jnp.where(pick, value, 0.0)
        return wide.reshape(groups * capacity, rows).astype(BF16)

    return spread(1.0), spread(high[:, None, :]), spread(low[:, None, :])


def route_kernel(count, groups, members, capacity, *refs):
    far, (out, high, low) = refs[: 2 * count], refs[2 * count : 2 * count + 3]
    near, sems = refs[2 * count + 3 : 4 * count + 3], refs[4 * count + 3]
    arrive = fetch(list(zip(far, near)), sems)
    mine = lax.axis_index("tensor").astype(F32)
    rows = high.shape[2]
    for i in range(count):
        arrive[i].wait()
        onehot, high[i], low[i] = weigh(near[i][...], (groups, capacity, rows), mine, members)
        arrive[count + i].wait()
        sent = dot(onehot, near[count + i][...]).astype(BF16)
        out[:, i * capacity : (i + 1) * capacity] = sent.reshape(groups, capacity, -1)


def route(metas, blocks, groups, members, capacity):
    count = len(blocks)
    rows, width = blocks[0].shape
    weights = jax.ShapeDtypeStruct((count, groups * capacity, rows), BF16)
    return pl.pallas_call(
        functools.partial(route_kernel, count, groups, members, capacity),
        out_shape=(
            jax.ShapeDtypeStruct((groups, count * capacity, width), BF16),
            weights,
            weights,
        ),
        in_specs=[HBM] * (2 * count),
        out_specs=(VMEM, VMEM, VMEM),
        scratch_shapes=[pltpu.VMEM(m.shape, F32) for m in metas]
        + [pltpu.VMEM(p.shape, BF16) for p in blocks]
        + [pltpu.SemaphoreType.DMA((2 * count,))],
        compiler_params=pltpu.CompilerParams(vmem_limit_bytes=LARGE),
        cost_estimate=pl.CostEstimate(
            flops=2 * count * groups * capacity * rows * width,
            bytes_accessed=count * (rows + groups * capacity) * width * 2,
            transcendentals=0,
        ),
        name="route",
    )(*metas, *blocks)


def pieces(total, size):
    starts = list(range(0, total - size + 1, size))
    ends = starts[1:] + [total]
    return list(zip(starts, ends))


AHEAD = 3


def mlp_kernel(fs, ns, block, turned, count, splits, *refs):
    xs, (wg, wu, wd) = refs[:count], refs[count : count + 3]
    outs, scratch = refs[count + 3 : count + 3 + splits], refs[count + 3 + splits :]
    x, vg, vu, vd, hidden, result, sems, x_sem = scratch
    total = x.shape[0]
    rows = total // count
    height = result.shape[1]
    copies = []
    for i, (a, b) in enumerate(fs):
        part = pl.ds(a, b - a) if turned else (slice(None), pl.ds(a, b - a))
        copies.append(
            (
                pltpu.make_async_copy(wg.at[part], vg.at[part], sems.at[0, i]),
                pltpu.make_async_copy(wu.at[part], vu.at[part], sems.at[1, i]),
            )
        )
    for i, (a, b) in enumerate(ns):
        part = (slice(None), pl.ds(a, b - a))
        copies.append((pltpu.make_async_copy(wd.at[part], vd.at[part], sems.at[2, i]),))

    def begin(i):
        if i < len(copies):
            for c in copies[i]:
                c.start()

    arrive = fetch([(xs[i], x.at[pl.ds(i * rows, rows)]) for i in range(count)], x_sem)
    for i in range(AHEAD):
        begin(i)
    finish(arrive)

    def over_rows(body):
        @pl.loop(0, total // block)
        def _(r):
            body(r, pl.ds(pl.multiple_of(r * block, block), block))

    for i, (a, b) in enumerate(fs):
        finish(copies[i])
        begin(i + AHEAD)

        def first(r, part):
            if turned:
                gate, up = ndot(x[part, :], vg[a:b, :]), ndot(x[part, :], vu[a:b, :])
            else:
                gate, up = dot(x[part, :], vg[:, a:b]), dot(x[part, :], vu[:, a:b])
            hidden[part, a:b] = (gate / (1.0 + jnp.exp(-gate)) * up).astype(BF16)

        over_rows(first)

    leave = []
    for i, (a, b) in enumerate(ns):
        finish(copies[len(fs) + i])
        begin(len(fs) + i + AHEAD)

        def second(r, part):
            value = dot(hidden[part, :], vd[:, a:b]).astype(BF16)
            several = block // height
            result[pl.ds(r * several, several), :, a:b] = value.reshape(several, height, b - a)

        over_rows(second)
        piece = height // splits
        for j in range(splits):
            leave.append(
                pltpu.make_async_copy(
                    result.at[:, pl.ds(j * piece, piece), pl.ds(a, b - a)],
                    outs[j].at[:, :, pl.ds(a, b - a)],
                    sems.at[j, i],
                )
            )
            leave[-1].start()
    finish(leave)


def mlp(xs, height, splits, wg, wu, wd, turned):
    width = xs[0].shape[1]
    total = sum(x.shape[0] for x in xs)
    inner = wd.shape[0]
    fs = pieces(inner, 256)
    ns = pieces(width, 512)
    out = jax.ShapeDtypeStruct((total // height, height // splits, width), BF16)
    return pl.pallas_call(
        functools.partial(mlp_kernel, fs, ns, 256, turned, len(xs), splits),
        out_shape=(out,) * splits,
        in_specs=[HBM] * (len(xs) + 3),
        out_specs=(HBM,) * splits,
        scratch_shapes=[
            pltpu.VMEM((total, width), BF16),
            pltpu.VMEM(wg.shape, BF16),
            pltpu.VMEM(wu.shape, BF16),
            pltpu.VMEM((inner, width), BF16),
            pltpu.VMEM((total, inner), BF16),
            pltpu.VMEM((total // height, height, width), BF16),
            pltpu.SemaphoreType.DMA((3, max(len(fs), len(ns)))),
            pltpu.SemaphoreType.DMA((len(xs),)),
        ],
        compiler_params=pltpu.CompilerParams(vmem_limit_bytes=LARGE),
        cost_estimate=pl.CostEstimate(
            flops=6 * total * width * inner,
            bytes_accessed=6 * width * inner + 4 * total * width,
            transcendentals=total * inner,
        ),
    )(*xs, wg, wu, wd)


def combine_kernel(order, final, *refs):
    count = len(order)
    inputs = 5 + count + final
    far, outs, scratch = refs[:inputs], refs[inputs : inputs + count], refs[inputs + count :]
    near, sems = scratch[:inputs], scratch[inputs]
    pairs = []
    for i in range(inputs):
        if i == 4:
            for j, d in enumerate(order):
                pairs.append((far[i].at[d], near[i].at[j]))
        else:
            pairs.append((far[i], near[i]))
    finish(fetch(pairs, sems))
    high, low, back, vector, shared = near[:5]
    tokens, others = near[5 : 5 + count], near[5 + count :]
    groups, height, width = back.shape
    capacity = height // count
    for i in range(count):
        logit = jnp.sum(
            tokens[i][...].astype(F32) * vector[...].astype(F32), axis=1, keepdims=True
        )
        scale = 1.0 / (1.0 + jnp.exp(-logit))
        part = back[:, i * capacity : (i + 1) * capacity].reshape(groups * capacity, width)
        total = tdot(high[i], part) + tdot(low[i], part) + scale * shared[i].astype(F32)
        for other in others:
            total = total + other[...].astype(F32)
        outs[i][...] = total.astype(BF16)


def combine(high, low, back, order, tokens, rows, vector, shared, others):
    count = len(order)
    width = back.shape[2]
    block = pltpu.VMEM((rows, width), BF16)
    return pl.pallas_call(
        functools.partial(combine_kernel, order, len(others)),
        out_shape=tuple(jax.ShapeDtypeStruct((rows, width), BF16) for _ in order),
        in_specs=[HBM] * (5 + count + len(others)),
        out_specs=tuple(VMEM for _ in order),
        scratch_shapes=[
            pltpu.VMEM(high.shape, BF16),
            pltpu.VMEM(low.shape, BF16),
            pltpu.VMEM(back.shape, BF16),
            pltpu.VMEM(vector.shape, BF16),
            pltpu.VMEM((count, rows, width), BF16),
        ]
        + [block] * (count + len(others))
        + [pltpu.SemaphoreType.DMA((4 + 2 * count + len(others),))],
        compiler_params=pltpu.CompilerParams(vmem_limit_bytes=LARGE),
        cost_estimate=pl.CostEstimate(
            flops=4 * back.size * rows // count,
            bytes_accessed=2 * back.size + 8 * count * rows * width,
            transcendentals=0,
        ),
    )(high, low, back, vector, shared, *tokens, *others)


def per_device(
    tokens, expert_ids, gate_probs, w_gate, w_up, w_down, s_gate, s_up, s_down, shared_gate
):
    rows, width = tokens.shape
    top = expert_ids.shape[1]
    groups = lax.axis_size("expert")
    members = lax.axis_size("tensor")
    capacity = max(2, 2 * top * rows // (groups * members))
    vector = shared_gate.reshape(1, width)

    def shift(x, d):
        return lax.ppermute(x, "tensor", [(i, (i + d) % members) for i in range(members)])

    def exchange(x):
        return lax.all_to_all(x, "expert", 0, 0, tiled=True)

    blocks, metas = {0: tokens}, {}
    metas[0] = jnp.concatenate([expert_ids.T.astype(F32), gate_probs.T], axis=0)
    for d in (1, 3, 2):
        blocks[d] = shift(tokens, -d)
        metas[d] = shift(metas[0], -d)

    def dispatch(chunk):
        sent, high, low = route(
            [metas[d] for d in chunk],
            [blocks[d] for d in chunk],
            groups,
            members,
            capacity,
        )
        return exchange(sent), high, low

    def expert(x, splits):
        flat = x.reshape(-1, width)
        return mlp([flat], x.shape[1], splits, w_gate[0], w_up[0], w_down[0], False)

    side, side_high, side_low = dispatch((1, 3))
    rest, rest_high, rest_low = dispatch((0, 2))
    shared = mlp(
        [blocks[d] for d in range(members)], rows, 1, s_gate.T, s_up.T, s_down, True
    )[0]
    (side,) = expert(side, 1)
    own, far = expert(rest, 2)
    back = exchange(side)
    first, third = combine(
        side_high,
        side_low,
        back,
        (1, 3),
        [blocks[1], blocks[3]],
        rows,
        vector,
        shared,
        [],
    )
    received = [shift(first, 1), shift(third, 3)]
    back = exchange(far)
    (second,) = combine(
        rest_high[1:], rest_low[1:], back, (2,), [blocks[2]], rows, vector, shared, []
    )
    received.append(shift(second, 2))
    back = exchange(own)
    return combine(
        rest_high[:1],
        rest_low[:1],
        back,
        (0,),
        [tokens],
        rows,
        vector,
        shared,
        received,
    )[0]


def solution(mesh):
    return jax.shard_map(
        per_device,
        mesh=mesh,
        in_specs=(
            P(("dp", "expert", "tensor"), None),
            P(("dp", "expert", "tensor"), None),
            P(("dp", "expert", "tensor"), None),
            P(("expert", "tensor"), None, None),
            P(("expert", "tensor"), None, None),
            P(("expert", "tensor"), None, None),
            P(None, "tensor"),
            P(None, "tensor"),
            P("tensor", None),
            P(),
        ),
        out_specs=P(("dp", "expert", "tensor"), None),
        check_vma=False,
    )
```
